32 devices in a mesh: dev: 32 (over z, y, x, core).
Axes of the slice: x: 2, y: 2, z: 4, core: 2. Of those that a mesh axis runs over, the one named last changes fastest.
Arguments:
- dual_blocks: bfloat16 [32, 3072, 3072], P('dev'), as said below
- rigid_modes: float32 [32, 6, 3072], P('dev'), may hold values from -5 to 5
- dual_local: float32 [32, 8, 3072], P('dev'), may hold values from -6 to 6
- coarse_rhs: float32 [32, 6, 8], P('dev'), may hold values from -4608 to 4608
- iface_sizes: int32 [32], P('dev'), may hold values from 1536 to 3072, as said below
- neighbours: int32 [32, 6], P('dev'), may hold values from -1 to 31, as said below
- shared_counts: int32 [32, 6], P('dev'), may hold values from 256 to 512, as said below
- iface_map: int32 [32, 3072], P('dev'), may hold values from -1 to 3071, as said below
- owner: int32 [32], replicated, may hold values from 0 to 31, as said below
Outputs:
- multipliers: float32 [32, 8, 3072], P('dev')
- projected_residual: float32 [32, 8, 3072], P('dev')
The draws below stay inside these ranges and needn't reach their ends.
Inputs may be any that keep to these rules, and one draw needn't show every extreme that they name: `dual_blocks`: each block is symmetric positive definite, and so is each of its leading principal parts. Grid subdomain g is held by slot owner[g] = (g + s) mod 32 for one offset s of the draw, so the subdomains across the faces -x, +x, -y, +y, -z, +z of slot i sit in slots i - 1, i + 1, i - 4, i + 4, i - 16, i + 16, taken mod 32. `neighbours`: the subdomains form a grid of 4 x 4 x 32/16 with g = x + 4 y + 16 z. Row i lists, for the faces -x, +x, -y, +y, -z, +z of the subdomain held in slot i, the grid subdomain across that face, or -1 on the outer boundary; across a face from g the opposite face names g. `shared_counts`: equal on both sides of a shared face; some subdomain has 512 on all its faces. `iface_sizes`: the sum of the slot's shared_counts row; some subdomain has 3072. `iface_map`: for j < iface_sizes[i], entry j is f * 512 + p for the dof at position p of face f of slot i (p below that face's count), each such code once; -1 beyond. The dof at position p of a shared face pairs with the dof at position p of the opposite face of the neighbour.
All inputs are finite; a program needn't handle non-finite values.
Results may differ from the reference program's by a relative error of at most 0.025.
Values sent between devices are 32-bit elements; how exact they have to be, the bound alone decides.
No kernel may reach another device: no remote copies, remote signals or barrier semaphores. Data moves between devices by JAX's collectives and lax.ppermute only.
A program may use at most 128 MiB of HBM per device.

```python
import math
import jax
import jax.numpy as jnp
from jax import lax

FACES = 6
MODES = 6
CAP = 512
NMAX = 3072
LOADS = 8
ITERS = 3
NSUB = 32


def grid_links():
    layers = NSUB // 16
    identity = jnp.arange(NSUB, dtype=jnp.int32)
    along_x = identity % 4
    along_y = identity // 4 % 4
    along_z = identity // 16
    columns = [jnp.where(along_x > 0, identity - 1, -1), jnp.where(along_x < 3, identity + 1, -1), jnp.where(along_y > 0, identity - 4, -1), jnp.where(along_y < 3, identity + 4, -1), jnp.where(along_z > 0, identity - 16, -1), jnp.where(along_z < layers - 1, identity + 16, -1)]
    return jnp.stack(columns, axis=1).astype(jnp.int32)


def layout_draw(key):
    base = jax.random.fold_in(key, 7301)
    key_count, key_star, key_owner, key_order = jax.random.split(base, 4)
    links = grid_links()
    drawn = jax.random.randint(key_count, (NSUB, FACES), CAP // 2, CAP + 1, dtype=jnp.int32)
    star = jax.random.randint(key_star, (), 0, NSUB, dtype=jnp.int32)
    drawn = drawn.at[star].set(CAP)
    for lower_face in (0, 2, 4):
        across = links[star, lower_face]
        drawn = drawn.at[jnp.where(across < 0, star, across), lower_face + 1].set(CAP)
    counts = drawn
    for lower_face in (0, 2, 4):
        across = links[:, lower_face]
        mirrored = drawn[jnp.clip(across, 0, NSUB - 1), lower_face + 1]
        counts = counts.at[:, lower_face].set(jnp.where(across < 0, drawn[:, lower_face], mirrored))
    offset = jax.random.randint(key_owner, (), 1, NSUB, dtype=jnp.int32)
    identity = jnp.arange(NSUB, dtype=jnp.int32)
    owner = ((identity + offset) % NSUB).astype(jnp.int32)
    hosted = ((identity - offset + NSUB) % NSUB).astype(jnp.int32)
    slot_links = links[hosted]
    slot_counts = counts[hosted]
    sizes = jnp.sum(slot_counts, axis=1).astype(jnp.int32)
    codes_all = jnp.arange(FACES * CAP, dtype=jnp.int32)
    live_codes = (codes_all % CAP)[None, :] < slot_counts[:, codes_all // CAP]
    slot_keys = jax.random.split(key_order, NSUB)
    shuffles = jax.vmap(lambda slot_key: jax.random.permutation(slot_key, FACES * CAP))(slot_keys).astype(jnp.int32)
    scores = shuffles + jnp.where(live_codes, 0, FACES * CAP).astype(jnp.int32)
    ordered = jnp.argsort(scores, axis=1, stable=True).astype(jnp.int32)
    positions = jnp.arange(NMAX, dtype=jnp.int32)
    iface_map = jnp.where(positions[None, :] < sizes[:, None], ordered, -1).astype(jnp.int32)
    return (owner, sizes, slot_links, slot_counts, iface_map, hosted)


def draw_owner(key, part):
    return layout_draw(key)[0]


def draw_iface_sizes(key, part):
    return layout_draw(key)[1]


def draw_neighbours(key, part):
    return layout_draw(key)[2]


def draw_shared_counts(key, part):
    return layout_draw(key)[3]


def draw_iface_map(key, part):
    return layout_draw(key)[4]


def mode_sample(sample_key, shape):
    values = jnp.clip(jax.random.normal(sample_key, shape, jnp.float32), -4.0, 4.0)
    return values


def draw_rigid_modes(key, part):
    owner, sizes, slot_links, slot_counts, iface_map, hosted = layout_draw(key)
    base = jax.random.fold_in(key, 7303)
    key_common, key_edge, key_own = jax.random.split(base, 3)
    common = mode_sample(key_common, (NSUB, 3, MODES, CAP))
    edge = mode_sample(key_edge, (NSUB, FACES, MODES, CAP))
    own = mode_sample(key_own, (NSUB, MODES, NMAX))
    face_ids = jnp.arange(FACES, dtype=jnp.int32)
    upper = face_ids % 2 == 1
    face_key = jnp.where(upper[None, :], hosted[:, None], slot_links)
    face_key = jnp.clip(face_key, 0, NSUB - 1).astype(jnp.int32)
    axis_ids = (face_ids // 2).astype(jnp.int32)
    face_vals = common[face_key, axis_ids[None, :]]
    face_vals = jnp.where((slot_links >= 0)[:, :, None, None], face_vals, edge)
    flattened = jnp.transpose(face_vals, (0, 2, 1, 3)).reshape(NSUB, MODES, FACES * CAP)
    codes = jnp.clip(iface_map, 0, FACES * CAP - 1).astype(jnp.int32)
    gather_index = jnp.broadcast_to(codes[:, None, :], (NSUB, MODES, NMAX))
    picked = jnp.take_along_axis(flattened, gather_index, axis=2)
    return (picked + 0.25 * own).astype(jnp.float32)


def draw_dual_blocks(key, part):
    slot_keys = jax.random.split(jax.random.fold_in(key, 7302), NSUB)
    spread = 0.3 / math.sqrt(NMAX)

    def single(slot_key):
        key_off, key_diag = jax.random.split(slot_key)
        entries = jax.random.normal(key_off, (NMAX, NMAX), jnp.float32)
        symmetric = (entries + entries.T) * (spread / math.sqrt(2.0))
        diag_vals = jax.random.uniform(key_diag, (NMAX,), jnp.float32, 1.0, 1.5)
        return (symmetric + jnp.diag(diag_vals)).astype(jnp.bfloat16)
    return jax.lax.map(single, slot_keys)


def block_levels(stream_key, shape, shards, smallest, largest):
    loudness, own = 1.0, jax.random.fold_in(stream_key, 6)
    for dim, shards_of in shards:
        steps = jnp.exp(jax.random.uniform(jax.random.fold_in(own, dim), (shards_of,), jnp.float32, smallest / len(shards), largest / len(shards)))
        loudness = loudness * jnp.repeat(steps, shape[dim] // shards_of).reshape([-1 if axis == dim else 1 for axis in range(len(shape))])
    return loudness


def normal_values(stream_key, extent, scale, bound, cuts=(), kind=jnp.bfloat16):
    values = scale * jax.random.normal(stream_key, extent, jnp.float32)
    if cuts:
        values = values * block_levels(stream_key, extent, cuts, -0.22, 0.18)
    return jnp.clip(values, -bound, bound).astype(kind)


def setup_inputs(seed: int = 0) -> dict:
    key_list = jax.random.split(jax.random.key(seed), 10)
    dual_blocks = draw_dual_blocks(jax.random.fold_in(key_list[9], 71), 0)
    rigid_modes = draw_rigid_modes(jax.random.fold_in(key_list[9], 71), 0)
    dual_local = normal_values(key_list[2], (NSUB, LOADS, NMAX), 1.0, 6.0, ((0, 32),), jnp.float32)
    coarse_rhs = normal_values(key_list[3], (NSUB, MODES, LOADS), (NMAX // 4), 4608.0, ((0, 32),), jnp.float32)
    iface_sizes = draw_iface_sizes(jax.random.fold_in(key_list[9], 71), 0)
    neighbours = draw_neighbours(jax.random.fold_in(key_list[9], 71), 0)
    shared_counts = draw_shared_counts(jax.random.fold_in(key_list[9], 71), 0)
    iface_map = draw_iface_map(jax.random.fold_in(key_list[9], 71), 0)
    owner = draw_owner(jax.random.fold_in(key_list[9], 71), 0)
    return {"dual_blocks": dual_blocks, "rigid_modes": rigid_modes, "dual_local": dual_local, "coarse_rhs": coarse_rhs, "iface_sizes": iface_sizes, "neighbours": neighbours, "shared_counts": shared_counts, "iface_map": iface_map, "owner": owner}


OPPOSITE = (1, 0, 3, 2, 5, 4)
HIGHEST_PRECISION = lax.Precision.HIGHEST

def tables(iface_sizes, neighbours, shared_counts, iface_map, owner):
    columns = jnp.arange(NMAX, dtype=jnp.int32)
    live_dofs = columns[None, :] < iface_sizes[:, None]
    dof_codes = jnp.clip(jnp.where(live_dofs, iface_map, 0), 0, FACES * CAP - 1).astype(jnp.int32)
    which_face = dof_codes // CAP
    position = dof_codes % CAP
    face_owner = jnp.take_along_axis(neighbours, which_face, axis=1)
    face_count = jnp.take_along_axis(shared_counts, which_face, axis=1)
    shared = live_dofs & (face_owner >= 0) & (position < face_count)
    weights = jnp.where(shared, 0.5, jnp.where(live_dofs, 1.0, 0.0)).astype(jnp.float32)
    row_index = jnp.broadcast_to(jnp.arange(NSUB, dtype=jnp.int32)[:, None], (NSUB, NMAX))
    targets = jnp.where(live_dofs, dof_codes, FACES * CAP).astype(jnp.int32)
    inverse = jnp.full((NSUB, FACES * CAP), NMAX, jnp.int32)
    inverse = inverse.at[row_index, targets].set(jnp.broadcast_to(columns[None, :], (NSUB, NMAX)), mode='drop')
    partner_slot = jnp.where(neighbours >= 0, owner[jnp.clip(neighbours, 0, NSUB - 1)], 0).astype(jnp.int32)
    face_mask = ((neighbours >= 0)[:, :, None] & (jnp.arange(CAP, dtype=jnp.int32)[None, None, :] < shared_counts[:, :, None])).astype(jnp.float32)
    return (live_dofs, dof_codes, shared, weights, inverse, partner_slot, face_mask)

def to_faces(values, inverse):
    padded = jnp.concatenate([values, jnp.zeros((values.shape[0], values.shape[1], 1), values.dtype)], axis=2)
    gather_index = jnp.broadcast_to(inverse[:, None, :], (values.shape[0], values.shape[1], FACES * CAP))
    return jnp.take_along_axis(padded, gather_index, axis=2).reshape(values.shape[0], values.shape[1], FACES, CAP)

def partner_faces(face_vals, partner_slot, face_mask):
    opposite = jnp.array(OPPOSITE, jnp.int32)
    swapped = jnp.transpose(face_vals, (0, 2, 1, 3))
    picked = swapped[partner_slot, opposite[None, :]]
    return picked * face_mask[:, :, None, :]

def to_dofs(far_faces, dof_codes, shared):
    flattened = jnp.transpose(far_faces, (0, 2, 1, 3)).reshape(far_faces.shape[0], far_faces.shape[2], FACES * CAP)
    gather_index = jnp.broadcast_to(dof_codes[:, None, :], (far_faces.shape[0], far_faces.shape[2], NMAX))
    return jnp.take_along_axis(flattened, gather_index, axis=2) * shared.astype(jnp.float32)[:, None, :]

def assemble(values, layout):
    live_dofs, dof_codes, shared, weights, inverse, partner_slot, face_mask = layout
    far_faces = partner_faces(to_faces(values, inverse), partner_slot, face_mask)
    return live_dofs.astype(jnp.float32)[:, None, :] * (values - to_dofs(far_faces, dof_codes, shared))

def dual_products(dual_blocks, vectors):

    def single(operands):
        dual_block, vector = operands
        return lax.dot_general(vector.astype(jnp.bfloat16).astype(jnp.float32), dual_block.astype(jnp.float32), (((1,), (1,)), ((), ())), preferred_element_type=jnp.float32)
    return lax.map(single, (dual_blocks, vectors))

def solve_coarse(factor, vector):
    middle = lax.linalg.triangular_solve(factor, vector, left_side=True, lower=True)
    return lax.linalg.triangular_solve(factor, middle, left_side=True, lower=True, transpose_a=True)

def weighted_inner(weights, left_vec, right_vec):
    return jnp.sum(weights[:, None, :] * left_vec * right_vec, axis=(0, 2))

def reference(dual_blocks, rigid_modes, dual_local, coarse_rhs, iface_sizes, neighbours, shared_counts, iface_map, owner):
    layout = tables(iface_sizes, neighbours, shared_counts, iface_map, owner)
    live_dofs, dof_codes, shared, weights, inverse, partner_slot, face_mask = layout
    live_float = live_dofs.astype(jnp.float32)
    modes_live = rigid_modes * live_float[:, None, :]
    own_modes = to_faces(modes_live, inverse)
    far_modes = partner_faces(own_modes, partner_slot, face_mask)
    diagonal = jnp.einsum('iaj,ibj->iab', modes_live, modes_live, precision=HIGHEST_PRECISION)
    coupling = -jnp.einsum('iafp,ifbp->ifab', own_modes, far_modes, precision=HIGHEST_PRECISION)
    slot_index = jnp.arange(NSUB, dtype=jnp.int32)
    coarse_blocks = jnp.zeros((NSUB, MODES, NSUB, MODES), jnp.float32)
    coarse_blocks = coarse_blocks.at[slot_index, :, slot_index, :].set(diagonal)
    coarse_blocks = coarse_blocks.at[slot_index[:, None], :, partner_slot, :].add(coupling)
    factor = jnp.linalg.cholesky(coarse_blocks.reshape(NSUB * MODES, NSUB * MODES))

    def modes_apply(solution):
        stacked = solution.reshape(NSUB, MODES, LOADS)
        own_part = jnp.einsum('iaj,ial->ilj', modes_live, stacked, precision=HIGHEST_PRECISION)
        return assemble(own_part, layout)

    def project(residual):
        coarse_all = jnp.einsum('iaj,ilj->ial', modes_live, residual, precision=HIGHEST_PRECISION).reshape(NSUB * MODES, LOADS)
        projected = residual - modes_apply(solve_coarse(factor, coarse_all))
        return (projected, weighted_inner(weights, projected, projected))

    def dual_apply(vector):
        return assemble(dual_products(dual_blocks, vector), layout)
    dual_rhs = assemble(dual_local, layout)
    multipliers = modes_apply(solve_coarse(factor, coarse_rhs.reshape(NSUB * MODES, LOADS)))
    residual = dual_rhs - dual_apply(multipliers)
    projected, norm_sq = project(residual)
    direction = projected
    for step_index in range(ITERS):
        applied = dual_apply(direction)
        step_size = norm_sq / weighted_inner(weights, direction, applied)
        multipliers = multipliers + step_size[None, :, None] * direction
        residual = residual - step_size[None, :, None] * applied
        projected, norm_next = project(residual)
        direction = projected + (norm_next / norm_sq)[None, :, None] * direction
        norm_sq = norm_next
    return (multipliers, projected)
```

```python
import functools

import jax
import jax.numpy as jnp
from jax import lax
from jax.experimental import pallas as pl
from jax.experimental.pallas import tpu as pltpu
from jax.sharding import PartitionSpec as P

HI = lax.Precision.HIGHEST
F32 = jnp.float32
STEPS = (-1, 1, -4, 4, -16, 16)
LANES = 128
PAD = 8
EXTRA = 64
SLOT, SHIFT, SIZE, COUNT, LINK = 0, 1, 2, 3, 9


def pairings(n):
    out = []
    for axis, dist in enumerate((1, 4, 16)):
        seen = []
        for phase in (0, 1):
            pairs = sorted({tuple(sorted((i, (i + dist) % n))) for i in range(n) if (i // dist) % 2 == phase})
            if pairs in seen:
                continue
            seen.append(pairs)
            out.append((axis, phase, pairs + [(j, i) for i, j in pairs]))
    merged = [sum(1 for a, _, _ in out if a == axis) == 1 for axis in range(3)]
    return out, merged


def dot(a, b, dims=((1,), (0,)), precision=HI):
    return lax.dot_general(a, b, (dims, ((), ())), precision=precision, preferred_element_type=F32)


def iota(shape, dim):
    return lax.broadcasted_iota(jnp.int32, shape, dim)


def take(x, idx):
    return jnp.take_along_axis(x, idx, axis=1, mode="promise_in_bounds")


def permute(load, table, blocks):
    tiles = [load(b) for b in range(blocks)]
    out = []
    for b in range(blocks):
        row = jnp.broadcast_to(table[b : b + 1, :], (8, LANES))
        high, low = row >> 7, row & 127
        acc = jnp.zeros((8, LANES), F32)
        for s in range(blocks):
            acc = jnp.where(high == s, take(tiles[s], low), acc)
        out.append(acc)
    return out


def tile_of(ref):
    return lambda b: ref[:, b * LANES : (b + 1) * LANES]


class Faces:
    def __init__(self, sc, n, cap):
        self.sc, self.n, self.cap = sc, n, cap
        self.per = cap // LANES
        self.list, self.merged = pairings(n)

    def bit(self, axis):
        return (self.sc[SLOT] >> (0, 2, 4)[axis]) & 1

    def live(self, f, t):
        return iota((8, LANES), 1) + t * LANES < self.sc[COUNT + f]

    def shared(self, f, t):
        return self.live(f, t) & (self.sc[LINK + f] > 0)

    def send(self, tiles, outs):
        for ref, (axis, phase, _) in zip(outs, self.list):
            up = self.sc[LINK + 2 * axis + 1] > 0 if self.merged[axis] else self.bit(axis) == phase
            for t in range(self.per):
                low, high = tiles[2 * axis * self.per + t], tiles[(2 * axis + 1) * self.per + t]
                ref[:, t * LANES : (t + 1) * LANES] = jnp.where(up, high, low)

    def far(self, ins, f, t):
        axis = f // 2
        mine = [ref for ref, (a, _, _) in zip(ins, self.list) if a == axis]
        vals = [ref[:, t * LANES : (t + 1) * LANES] for ref in mine]
        if len(vals) == 1:
            v = vals[0]
        else:
            zero = self.bit(axis) == 0
            v = jnp.where(zero, vals[0], vals[1]) if f % 2 else jnp.where(zero, vals[1], vals[0])
        return jnp.where(self.shared(f, t), v, 0.0)


def spread(n, width):
    row, col = iota((LANES, width), 0), iota((LANES, width), 1)
    hit = jnp.zeros((LANES, width), jnp.bool_)
    for b, step in enumerate((0,) + STEPS):
        hit = hit | ((row >> 3 == b) & (col == (step % n) * PAD + (row & 7)))
    return jnp.where(hit, 1.0, 0.0).astype(F32)


def prepare_kernel(n, cap, faces, sc, map_row, map_tile, modes, rhs, *refs):
    nm = len(pairings(n)[0])
    modes_out, rhs_out, code_out, inv_out = refs[:4]
    sends, scratch = refs[4 : 4 + nm], refs[4 + nm]
    nmax = cap * faces
    blocks = nmax // LANES
    size = sc[SIZE]
    j = iota((1, nmax), 1)
    code = jnp.where(j < size, map_row[...], -1)
    place = j + 1
    high, low = code >> 7, code & 127
    rows = -(-blocks // 8) * 8
    group = iota((rows, nmax), 0)
    hit = jnp.broadcast_to(high, (rows, nmax)) == group
    left = jnp.concatenate(
        [
            jnp.where(hit, jnp.broadcast_to(place >> 6, (rows, nmax)), 0).astype(F32),
            jnp.where(hit, jnp.broadcast_to(place & 63, (rows, nmax)), 0).astype(F32),
        ],
        axis=0,
    ).astype(jnp.bfloat16)
    right = jnp.where(jnp.broadcast_to(low, (LANES, nmax)) == iota((LANES, nmax), 0), 1.0, 0.0).astype(jnp.bfloat16)
    both = dot(left, right, ((1,), (1,)), None)
    inv = (both[:rows] * 64.0 + both[rows:]).astype(jnp.int32) - 1
    inv_out[...] = inv[:blocks]
    tile_j = iota((blocks, LANES), 0) * LANES + iota((blocks, LANES), 1)
    code_out[...] = jnp.where(tile_j < size, map_tile[...], -1)
    scratch[...] = jnp.zeros_like(scratch)
    scratch[: modes.shape[1], :] = modes[0]
    moved = permute(tile_of(scratch), inv_out, blocks)
    for b, v in enumerate(moved):
        modes_out[:, b * LANES : (b + 1) * LANES] = v
    Faces(sc, n, cap).send(moved, sends)
    for b, v in enumerate(permute(lambda b: rhs[0, :, b * LANES : (b + 1) * LANES], inv_out, blocks)):
        rhs_out[:, b * LANES : (b + 1) * LANES] = v


def row_kernel(n, cap, faces, sc, modes, goal, *refs):
    nm = len(pairings(n)[0])
    ins, (c_out, tile_out) = refs[:nm], refs[nm:]
    fc = Faces(sc, n, cap)
    c_out[...] = jnp.zeros_like(c_out)
    c_out[0:PAD, :] = modes[...]
    for f in range(faces):
        for t in range(fc.per):
            at = f * cap + t * LANES
            c_out[PAD * (1 + f) : PAD * (2 + f), at : at + LANES] = -fc.far(ins, f, t)
    row = dot(modes[...], c_out[...], ((1,), (1,)))
    tile = jnp.concatenate([row, jnp.zeros((8, LANES - EXTRA), F32)], axis=1) + goal[...]
    for i in range(n):
        tile_out[i] = tile


def sweep(ref, side):
    cols = side // LANES
    reals = 6

    def step(b, carry):
        at = pl.multiple_of(b * PAD, PAD)
        column = pl.multiple_of((at // LANES) * LANES, LANES)
        lane0 = at - column
        sub, lane = iota((8, LANES), 0), iota((8, LANES), 1)
        rows = [ref[pl.ds(at, PAD), j * LANES : (j + 1) * LANES] for j in range(cols)]
        pivot = ref[pl.ds(at, PAD), pl.ds(column, LANES)]
        g = [take(pivot, jnp.full((8, LANES), 0, jnp.int32) + (lane0 + c)) for c in range(reals)]
        for k in range(reals):
            top = [jnp.broadcast_to(g[c][k : k + 1, :], (8, LANES)) for c in range(reals)]
            inv = 1.0 / top[k]
            mine = sub == k
            new = []
            for c in range(reals):
                if c == k:
                    new.append(jnp.where(mine, inv, -g[k] * inv))
                else:
                    scaled = top[c] * inv
                    new.append(jnp.where(mine, scaled, g[c] - g[k] * scaled))
            g = new
        w = []
        for j in range(cols):
            acc = jnp.zeros((8, LANES), F32)
            for c in range(reals):
                acc = acc + g[c] * jnp.broadcast_to(rows[j][c : c + 1, :], (8, LANES))
            here = (lane + j * LANES >= at) & (lane + j * LANES < at + reals)
            minus = acc
            for c in range(reals):
                minus = jnp.where(lane + j * LANES == at + c, -g[c], minus)
            w.append((minus, here))
        wb = [[jnp.broadcast_to(w[j][0][c : c + 1, :], (8, LANES)) for c in range(reals)] for j in range(cols)]
        for i in range(side // PAD):
            r = slice(i * PAD, (i + 1) * PAD)
            src = ref[r, pl.ds(column, LANES)]
            splat = [take(src, jnp.full((8, LANES), 0, jnp.int32) + (lane0 + c)) for c in range(reals)]
            for j in range(cols):
                x = jnp.where(w[j][1], 0.0, ref[r, j * LANES : (j + 1) * LANES])
                for c in range(reals):
                    x = x - splat[c] * wb[j][c]
                ref[r, j * LANES : (j + 1) * LANES] = x
        for j in range(cols):
            ref[pl.ds(at, PAD), j * LANES : (j + 1) * LANES] = jnp.where(sub < reals, w[j][0], rows[j])
        return carry

    lax.fori_loop(0, side // PAD, step, 0)


def place(tile, src, dst, width=PAD):
    moved = tile if src == dst else pltpu.roll(tile, (dst - src) % LANES, 1)
    lane = iota((8, LANES), 1)
    return jnp.where((lane >= dst) & (lane < dst + width), moved, 0.0)


def invert(n, sc, recv, dred, qrb, sbb):
    half = n // 2
    side = half * PAD
    cols = side // LANES
    shift = sc[SHIFT]
    layers = n // 16
    qrb[...] = jnp.zeros_like(qrb)
    sbb[...] = jnp.zeros_like(sbb)
    dred[...] = jnp.zeros_like(dred)
    for g in range(n):
        x, y, z = g % 4, g // 4 % 4, g // 16
        k = g // 2
        tile = recv[lax.rem(g + shift, n)]
        at = k * PAD
        own = slice((at // LANES) * LANES, (at // LANES + 1) * LANES)
        diag = place(tile, 0, at % LANES)
        if (x + y + z) % 2 == 0:
            dred[:, own] += diag
            there = (x > 0, x < 3, y > 0, y < 3, z > 0, z < layers - 1)
            parts = {}
            for f, step in enumerate(STEPS):
                if there[f]:
                    to = (g + step) // 2 * PAD
                    piece = place(tile, PAD * (1 + f), to % LANES)
                    parts[to // LANES] = parts[to // LANES] + piece if to // LANES in parts else piece
            for j, v in parts.items():
                qrb[at : at + PAD, j * LANES : (j + 1) * LANES] = v
        else:
            sbb[at : at + PAD, own] = diag
    sub, lane = iota((8, LANES), 0), iota((8, LANES), 1)
    padded = (sub >= 6) & (sub == (lane & 7))
    tred = []
    for j in range(cols):
        m = dred[:, j * LANES : (j + 1) * LANES]
        m = jnp.where(padded, 1.0, m)
        for k in range(6):
            col = take(m, (lane & ~7) + k)
            row = jnp.broadcast_to(m[k : k + 1, :], (8, LANES))
            inv = 1.0 / jnp.broadcast_to(col[k : k + 1, :], (8, LANES))
            scaled = row * inv
            in_col, in_row = (lane & 7) == k, sub == k
            m = jnp.where(
                in_row,
                jnp.where(in_col, inv, scaled),
                jnp.where(in_col, -col * inv, m - col * scaled),
            )
        tred.append(m)
    dd = jnp.concatenate(
        [
            jnp.concatenate([jnp.where((lane + j * LANES) >> 3 == k, tred[j], 0.0) for j in range(cols)], axis=1)
            for k in range(half)
        ],
        axis=0,
    )
    q = qrb[...]
    t = dot(dd, q)
    r, c = iota((side, side), 0), iota((side, side), 1)
    sbb[...] = jnp.where((r == c) & ((r & 7) >= 6), 1.0, sbb[...] - dot(q, t, ((0,), (0,))))
    sweep(sbb, side)
    sinv = -sbb[...]
    ts = dot(t, sinv)
    def slot_of(pos, black):
        twice = 2 * pos
        odd = ((twice >> 2) ^ (twice >> 4)) & 1
        g = twice + ((1 - odd) if black else odd)
        return lax.rem(g + shift, n)

    rr, cc = iota((side, LANES), 0), iota((side, LANES), 1)
    sel = []
    for black in (False, True):
        slot = slot_of(rr >> 3, black)
        hit = jnp.zeros((side, LANES), jnp.bool_)
        for b, step in enumerate((0,) + STEPS):
            hit = hit | ((cc >> 3 == b) & (slot == lax.rem(sc[SLOT] + step + n, n)))
        sel.append(jnp.where(hit & ((rr & 7) == (cc & 7)), 1.0, 0.0).astype(F32))
    upper = dot(dd, sel[0]) + dot(ts, dot(t, sel[0], ((0,), (0,)))) - dot(ts, sel[1])
    lower = dot(sinv, sel[1]) - dot(ts, sel[0], ((0,), (0,)))
    pr, pc = iota((n * PAD, side), 0), iota((n * PAD, side), 1)
    out = None
    for black, x in ((False, upper), (True, lower)):
        onehot = jnp.where((slot_of(pc >> 3, black) == pr >> 3) & ((pc & 7) == (pr & 7)), 1.0, 0.0).astype(F32)
        v = dot(onehot, x)
        out = v if out is None else out + v
    return out


class Product:
    def __init__(self, b_hbm, b_vmem, sems):
        self.chunks = b_vmem.shape[0]
        rows = b_vmem.shape[1]
        self.copies = [
            pltpu.make_async_copy(b_hbm.at[0, pl.ds(k * rows, rows), :], b_vmem.at[k], sems.at[k]) for k in range(self.chunks)
        ]
        self.b = b_vmem
        for c in self.copies:
            c.start()

    def __call__(self, tiles, code, inv, acc, vec):
        blocks = len(tiles)
        moved = permute(lambda b: tiles[b], code, blocks)
        per = blocks // self.chunks
        for k in range(self.chunks):
            v = jnp.concatenate(moved[k * per : (k + 1) * per], axis=1)
            high = v.astype(jnp.bfloat16)
            low = (v - high.astype(F32)).astype(jnp.bfloat16)
            vec[k] = jnp.concatenate([high, low], axis=0)
        for k in range(self.chunks):
            self.copies[k].wait()
            part = dot(vec[k], self.b[k], precision=None)
            acc[...] = part if k == 0 else acc[...] + part
        return permute(lambda b: acc[0:8, b * LANES : (b + 1) * LANES] + acc[8:16, b * LANES : (b + 1) * LANES], inv, blocks)


def lanes_of(ref, b):
    return ref[:, b * LANES : (b + 1) * LANES]


def weigh(fc, f, t, x):
    return jnp.where(fc.shared(f, t), 0.5, jnp.where(fc.live(f, t), 1.0, 0.0)) * x


def total(tiles):
    acc = tiles[0]
    for x in tiles[1:]:
        acc = acc + x
    return jnp.sum(acc, axis=1, keepdims=True)


def coarse_of(n, recv, qloc):
    width = n * PAD
    rows = jnp.concatenate([recv[i] for i in range(n)], axis=0)
    dense = dot(rows, spread(n, width))
    goal = None
    both = None
    for i in range(n):
        x = dense[i * 8 : (i + 1) * 8, :]
        x = x if i == 0 else pltpu.roll(x, i * PAD, 1)
        goal = x if goal is None else goal + x
        both = recv[i] if both is None else both + recv[i]
    return dot(goal, qloc[...])[:, :EXTRA], both


def finish(n, fc, y, extra, c_ref, ybuf, tile_out):
    for b, v in enumerate(y):
        ybuf[:, b * LANES : (b + 1) * LANES] = v
    row = dot(ybuf[...], c_ref[...], ((1,), (1,)))
    tile = jnp.concatenate([row, jnp.zeros((8, LANES - EXTRA), F32)], axis=1)
    lane = iota((8, LANES), 1)
    for k, v in enumerate(extra):
        tile = jnp.where(lane == EXTRA + k, v, tile)
    for i in range(n):
        tile_out[i] = tile


def start_kernel(n, cap, faces, sc, b_hbm, recv, c_ref, rhs, code, inv, *refs):
    nm = len(pairings(n)[0])
    lam_out, t_out, q_out, tile_out = refs[:4]
    sends = refs[4 : 4 + nm]
    b_vmem, sems, acc, vec, dred, qrb, sbb = refs[4 + nm :]
    product = Product(b_hbm, b_vmem, sems)
    fc = Faces(sc, n, cap)
    blocks = cap * faces // LANES
    q_out[...] = invert(n, sc, recv, dred, qrb, sbb)
    goal = []
    for j in range(n * PAD // LANES):
        v = None
        for i in range(j * (LANES // PAD), (j + 1) * (LANES // PAD)):
            x = place(recv[i], EXTRA, (i * PAD) % LANES)
            v = x if v is None else v + x
        goal.append(v)
    z = dot(jnp.concatenate(goal, axis=1), q_out[...])[:, :EXTRA]
    lam_out[...] = dot(z, c_ref[...])
    y = product([lanes_of(lam_out, b) for b in range(blocks)], code, inv, acc, vec)
    t = [lanes_of(rhs, b) - y[b] for b in range(blocks)]
    fc.send(t, sends)
    finish(n, fc, t, [], c_ref, t_out, tile_out)


def assembled(fc, faces, c_ref, z, y_ref, far, buf):
    buf[...] = dot(z, c_ref[...])
    out = []
    for f in range(faces):
        for t in range(fc.per):
            b = f * fc.per + t
            v = lanes_of(y_ref, b) - fc.far(far, f, t)
            out.append(jnp.where(fc.live(f, t), v, 0.0) - lanes_of(buf, b))
    return out


def step_kernel(n, cap, faces, kind, sc, b_hbm, recv, c_ref, q_ref, code, inv, y_ref, *refs):
    refs = list(refs)
    nm = len(pairings(n)[0])
    pop = lambda k: [refs.pop(0) for _ in range(k)]
    far = pop(nm)
    state = pop({0: 0, 1: 2, 2: 5, 3: 5}[kind])
    fc = Faces(sc, n, cap)
    blocks = cap * faces // LANES
    if kind == 3:
        x_out, w_out, buf = refs
    else:
        w_out = pop(1)[0]
        x_out, p_out, s_out, k_out = pop(4) if kind else (None,) * 4
        y_out, tile_out = pop(2)
        sends = pop(nm)
        b_vmem, sems, acc, vec, buf = refs
        product = Product(b_hbm, b_vmem, sems)
    z, both = coarse_of(n, recv, q_ref)
    q = assembled(fc, faces, c_ref, z, y_ref, far, buf)
    if kind == 0:
        w, p, s = q, None, None
    else:
        rho, mu = both[:, EXTRA : EXTRA + 1], both[:, EXTRA + 1 : EXTRA + 2]
        w_old = [lanes_of(state[0], b) for b in range(blocks)]
        x_old = [lanes_of(state[1], b) for b in range(blocks)]
        if kind == 1:
            p, s, sigma = w_old, q, mu
        else:
            last = state[4][...]
            beta = rho / last[:, 0:1]
            cross = both[:, EXTRA + 2 : EXTRA + 3]
            sigma = mu + beta * cross + beta * beta * last[:, 1:2]
            p = [w_old[b] + beta * lanes_of(state[2], b) for b in range(blocks)]
            s = [q[b] + beta * lanes_of(state[3], b) for b in range(blocks)]
        alpha = rho / sigma
        w = [w_old[b] - alpha * s[b] for b in range(blocks)]
        x = [x_old[b] + alpha * p[b] for b in range(blocks)]
        if kind == 3:
            for out, v in ((x_out, x), (w_out, w)):
                for b, m in enumerate(permute(lambda b: v[b], code, blocks)):
                    out[0, :, b * LANES : (b + 1) * LANES] = m
            return
        lane = iota((8, LANES), 1)
        k_out[...] = jnp.where(lane == 0, rho, jnp.where(lane == 1, sigma, 0.0))
        for b in range(blocks):
            at = slice(b * LANES, (b + 1) * LANES)
            x_out[:, at], p_out[:, at], s_out[:, at] = x[b], p[b], s[b]
    for b in range(blocks):
        w_out[:, b * LANES : (b + 1) * LANES] = w[b]
    y = product(w, code, inv, acc, vec)
    fc.send(y, sends)
    w = [lanes_of(w_out, b) for b in range(blocks)]
    weighted = [weigh(fc, b // fc.per, b % fc.per, w[b]) for b in range(blocks)]
    extra = [total([weighted[b] * w[b] for b in range(blocks)]), total([w[b] * y[b] for b in range(blocks)])]
    if kind:
        extra.append(total([weighted[b] * lanes_of(s_out, b) + lanes_of(p_out, b) * y[b] for b in range(blocks)]))
    finish(n, fc, y, extra, c_ref, y_out, tile_out)


VMEM = pl.BlockSpec(memory_space=pltpu.VMEM)
SMEM = pl.BlockSpec(memory_space=pltpu.SMEM)
ANY = pl.BlockSpec(memory_space=pl.ANY)


def struct(*shape, dtype=F32):
    return jax.ShapeDtypeStruct(shape, dtype)


def per_device(
    dual_blocks, rigid_modes, dual_local, coarse_rhs, iface_sizes, neighbours, shared_counts, iface_map, owner
):
    n = lax.axis_size("dev")
    faces = neighbours.shape[1]
    nmax = iface_map.shape[1]
    cap = nmax // faces
    modes, loads = coarse_rhs.shape[1:]
    blocks = nmax // LANES
    pairs, _ = pairings(n)
    nm = len(pairs)
    params = pltpu.CompilerParams(vmem_limit_bytes=56 * 1024 * 1024)
    sc = jnp.concatenate(
        [
            lax.axis_index("dev").astype(jnp.int32)[None],
            owner[:1],
            iface_sizes,
            shared_counts[0],
            (neighbours[0] >= 0).astype(jnp.int32),
        ]
    )
    goal = jnp.zeros((8, LANES), F32).at[:loads, EXTRA : EXTRA + modes].set(coarse_rhs[0].T)
    vec = struct(8, nmax)
    face = [struct(8, cap)] * nm
    tiles = struct(n, 8, LANES)
    table = struct(blocks, LANES, dtype=jnp.int32)

    def call(kernel, name, in_specs, outs, scratch, *args):
        return pl.pallas_call(
            kernel,
            out_shape=outs,
            in_specs=in_specs,
            out_specs=[VMEM] * len(outs),
            scratch_shapes=scratch,
            compiler_params=params,
            name=name,
        )(*args)

    def exchange(parts):
        return [lax.ppermute(x, "dev", perm) for x, (_, _, perm) in zip(parts, pairs)]

    def everyone(x):
        return lax.all_to_all(x, "dev", 0, 0)

    modes_c, rhs_c, code, inv, *send = call(
        functools.partial(prepare_kernel, n, cap, faces),
        "prepare",
        [SMEM] + [VMEM] * 4,
        [vec, vec, table, table] + face,
        [pltpu.VMEM((8, nmax), F32)],
        sc,
        iface_map,
        iface_map.reshape(blocks, LANES),
        rigid_modes,
        dual_local,
    )
    far = exchange(send)
    c_mat, tile = call(
        functools.partial(row_kernel, n, cap, faces),
        "coarse_row",
        [SMEM] + [VMEM] * (2 + nm),
        [struct(EXTRA, nmax), tiles],
        [],
        sc,
        modes_c,
        goal,
        *far,
    )
    recv = everyone(tile)
    chunk = 256
    dense = [
        pltpu.VMEM((nmax // chunk, chunk, nmax), jnp.bfloat16),
        pltpu.SemaphoreType.DMA((nmax // chunk,)),
        pltpu.VMEM((16, nmax), F32),
        pltpu.VMEM((nmax // chunk, 16, chunk), jnp.bfloat16),
    ]
    side = n * PAD // 2
    x, y, q_mat, tile, *send = call(
        functools.partial(start_kernel, n, cap, faces),
        "start",
        [SMEM, ANY] + [VMEM] * 5,
        [vec, vec, struct(n * PAD, LANES), tiles] + face,
        dense + [pltpu.VMEM((8, side), F32), pltpu.VMEM((side, side), F32), pltpu.VMEM((side, side), F32)],
        sc,
        dual_blocks,
        recv,
        c_mat,
        rhs_c,
        code,
        inv,
    )
    state = []
    for kind in (0, 1, 2, 3):
        recv, far = everyone(tile), exchange(send)
        args = (sc, dual_blocks, recv, c_mat, q_mat, code, inv, y, *far, *state)
        specs = [SMEM, ANY] + [VMEM] * (len(args) - 2)
        body = functools.partial(step_kernel, n, cap, faces, kind)
        buf = [pltpu.VMEM((8, nmax), F32)]
        if kind == 3:
            return tuple(call(body, "last", specs, [struct(1, 8, nmax)] * 2, buf, *args))
        outs = [vec] + ([vec, vec, vec, struct(8, LANES)] if kind else []) + [vec, tiles] + face
        got = list(call(body, f"step{kind}", specs, outs, dense + buf, *args))
        w = got.pop(0)
        if kind:
            x, p, s, scal = got[:4]
            got = got[4:]
            state = [w, x, p, s, scal]
        else:
            state = [w, x]
        y, tile, send = got[0], got[1], got[2:]


def solution(mesh):
    return jax.shard_map(
        per_device,
        mesh=mesh,
        in_specs=(
            P("dev", None, None),
            P("dev", None, None),
            P("dev", None, None),
            P("dev", None, None),
            P("dev"),
            P("dev", None),
            P("dev", None),
            P("dev", None),
            P(),
        ),
        out_specs=(P("dev", None, None), P("dev", None, None)),
        check_vma=False,
    )
```

```python
import functools

import jax
import jax.numpy as jnp
from jax import lax
from jax.experimental import pallas as pl
from jax.experimental.pallas import tpu as pltpu
from jax.sharding import PartitionSpec as P

HI = lax.Precision.HIGHEST
F32 = jnp.float32
STEPS = (-1, 1, -4, 4, -16, 16)
LANES = 128
PAD = 8
EXTRA = 64
SLOT, SHIFT, SIZE, COUNT, LINK = 0, 1, 2, 3, 9


def pairings(n):
    out = []
    for axis, dist in enumerate((1, 4, 16)):
        seen = []
        for phase in (0, 1):
            pairs = sorted({tuple(sorted((i, (i + dist) % n))) for i in range(n) if (i // dist) % 2 == phase})
            if pairs in seen:
                continue
            seen.append(pairs)
            out.append((axis, phase, pairs + [(j, i) for i, j in pairs]))
    merged = [sum(1 for a, _, _ in out if a == axis) == 1 for axis in range(3)]
    return out, merged


def dot(a, b, dims=((1,), (0,)), precision=HI):
    return lax.dot_general(a, b, (dims, ((), ())), precision=precision, preferred_element_type=F32)


def iota(shape, dim):
    return lax.broadcasted_iota(jnp.int32, shape, dim)


def take(x, idx):
    return jnp.take_along_axis(x, idx, axis=1, mode="promise_in_bounds")


def permute(load, table, blocks):
    tiles = [load(b) for b in range(blocks)]
    out = []
    for b in range(blocks):
        row = jnp.broadcast_to(table[b : b + 1, :], (8, LANES))
        high, low = row >> 7, row & 127
        acc = jnp.zeros((8, LANES), F32)
        for s in range(blocks):
            acc = jnp.where(high == s, take(tiles[s], low), acc)
        out.append(acc)
    return out


class Faces:
    def __init__(self, sc, n, cap):
        self.sc, self.n, self.cap = sc, n, cap
        self.per = cap // LANES
        self.list, self.merged = pairings(n)

    def bit(self, axis):
        return (self.sc[SLOT] >> (0, 2, 4)[axis]) & 1

    def live(self, f, t):
        return iota((8, LANES), 1) + t * LANES < self.sc[COUNT + f]

    def shared(self, f, t):
        return self.live(f, t) & (self.sc[LINK + f] > 0)

    def send(self, tiles, outs):
        for ref, (axis, phase, _) in zip(outs, self.list):
            up = self.sc[LINK + 2 * axis + 1] > 0 if self.merged[axis] else self.bit(axis) == phase
            for t in range(self.per):
                low, high = tiles[2 * axis * self.per + t], tiles[(2 * axis + 1) * self.per + t]
                ref[:, t * LANES : (t + 1) * LANES] = jnp.where(up, high, low)

    def far(self, ins, f, t):
        axis = f // 2
        mine = [ref for ref, (a, _, _) in zip(ins, self.list) if a == axis]
        vals = [ref[:, t * LANES : (t + 1) * LANES] for ref in mine]
        if len(vals) == 1:
            v = vals[0]
        else:
            zero = self.bit(axis) == 0
            v = jnp.where(zero, vals[0], vals[1]) if f % 2 else jnp.where(zero, vals[1], vals[0])
        return jnp.where(self.shared(f, t), v, 0.0)


def spread(n, width):
    row, col = iota((LANES, width), 0), iota((LANES, width), 1)
    hit = jnp.zeros((LANES, width), jnp.bool_)
    for b, step in enumerate((0,) + STEPS):
        hit = hit | ((row >> 3 == b) & (col == (step % n) * PAD + (row & 7)))
    return jnp.where(hit, 1.0, 0.0).astype(F32)


def prepare_kernel(n, cap, faces, owner, sizes, counts, links, map_row, map_tile, modes, rhs, sc, *refs):
    nm = len(pairings(n)[0])
    modes_out, rhs_out, code_out, inv_out = refs[:4]
    sends = refs[4 : 4 + nm]
    sc[SLOT] = lax.axis_index("dev").astype(jnp.int32)
    sc[SHIFT] = owner[0]
    sc[SIZE] = sizes[0]
    for f in range(faces):
        sc[COUNT + f] = counts[0, f]
        sc[LINK + f] = (links[0, f] >= 0).astype(jnp.int32)
    nmax = cap * faces
    blocks = nmax // LANES
    size = sc[SIZE]
    j = iota((1, nmax), 1)
    code = jnp.where(j < size, map_row[...], -1)
    place = j + 1
    high, low = code >> 7, code & 127
    rows = -(-blocks // 8) * 8
    group = iota((rows, nmax), 0)
    hit = jnp.broadcast_to(high, (rows, nmax)) == group
    left = jnp.concatenate(
        [
            jnp.where(hit, jnp.broadcast_to(place >> 6, (rows, nmax)), 0).astype(F32),
            jnp.where(hit, jnp.broadcast_to(place & 63, (rows, nmax)), 0).astype(F32),
        ],
        axis=0,
    ).astype(jnp.bfloat16)
    right = jnp.where(jnp.broadcast_to(low, (LANES, nmax)) == iota((LANES, nmax), 0), 1.0, 0.0).astype(jnp.bfloat16)
    both = dot(left, right, ((1,), (1,)), None)
    inv = (both[:rows] * 64.0 + both[rows:]).astype(jnp.int32) - 1
    inv_out[...] = inv[:blocks]
    tile_j = iota((blocks, LANES), 0) * LANES + iota((blocks, LANES), 1)
    code_out[...] = jnp.where(tile_j < size, map_tile[...], -1)
    count = modes.shape[0] // blocks
    rest = jnp.zeros((8 - count, LANES), F32)
    moved = permute(
        lambda b: jnp.concatenate([modes[pl.ds(b, count, blocks), :], rest], axis=0), inv_out, blocks
    )
    for b, v in enumerate(moved):
        modes_out[:, b * LANES : (b + 1) * LANES] = v
    Faces(sc, n, cap).send(moved, sends)
    for b, v in enumerate(permute(lambda b: rhs[0, :, b * LANES : (b + 1) * LANES], inv_out, blocks)):
        rhs_out[:, b * LANES : (b + 1) * LANES] = v


def row_kernel(n, cap, faces, sc, modes, goal, *refs):
    nm = len(pairings(n)[0])
    ins, (c_out, tile_out) = refs[:nm], refs[nm:]
    fc = Faces(sc, n, cap)
    c_out[...] = jnp.zeros_like(c_out)
    c_out[0:PAD, :] = modes[...]
    for f in range(faces):
        for t in range(fc.per):
            at = f * cap + t * LANES
            c_out[PAD * (1 + f) : PAD * (2 + f), at : at + LANES] = -fc.far(ins, f, t)
    row = dot(modes[...], c_out[...], ((1,), (1,)))
    count = goal.shape[0]
    onehot = jnp.where(iota((count, LANES), 1) == iota((count, LANES), 0) + EXTRA, 1.0, 0.0).astype(F32)
    tile = jnp.concatenate([row, jnp.zeros((8, LANES - EXTRA), F32)], axis=1) + dot(goal[...], onehot, ((0,), (0,)))
    for i in range(n):
        tile_out[i] = tile


def sweep(ref, side):
    cols = side // LANES
    reals = 6

    def step(b, carry):
        at = pl.multiple_of(b * PAD, PAD)
        column = 0 if cols == 1 else pl.multiple_of((at // LANES) * LANES, LANES)
        lane0 = at - column
        sub, lane = iota((8, LANES), 0), iota((8, LANES), 1)
        rows = [ref[pl.ds(at, PAD), j * LANES : (j + 1) * LANES] for j in range(cols)]
        pivot = rows[0] if cols == 1 else ref[pl.ds(at, PAD), pl.ds(column, LANES)]
        g = [take(pivot, jnp.full((8, LANES), 0, jnp.int32) + (lane0 + c)) for c in range(reals)]
        for k in range(reals):
            top = [jnp.broadcast_to(g[c][k : k + 1, :], (8, LANES)) for c in range(reals)]
            inv = 1.0 / top[k]
            mine = sub == k
            new = []
            for c in range(reals):
                if c == k:
                    new.append(jnp.where(mine, inv, -g[k] * inv))
                else:
                    scaled = top[c] * inv
                    new.append(jnp.where(mine, scaled, g[c] - g[k] * scaled))
            g = new
        w = []
        for j in range(cols):
            acc = jnp.zeros((8, LANES), F32)
            for c in range(reals):
                acc = acc + g[c] * jnp.broadcast_to(rows[j][c : c + 1, :], (8, LANES))
            here = (lane + j * LANES >= at) & (lane + j * LANES < at + reals)
            minus = acc
            for c in range(reals):
                minus = jnp.where(lane + j * LANES == at + c, -g[c], minus)
            w.append((minus, here))
        wb = [[jnp.broadcast_to(w[j][0][c : c + 1, :], (8, LANES)) for c in range(reals)] for j in range(cols)]
        if cols == 1:
            lanes = [jnp.full((8, LANES), 0, jnp.int32) + (lane0 + c) for c in range(reals)]
            olds = [ref[i * PAD : (i + 1) * PAD, :] for i in range(side // PAD)]
            splats = [[take(x, i) for i in lanes] for x in olds]
            for i, x in enumerate(olds):
                x = jnp.where(w[0][1], 0.0, x)
                for c in range(reals):
                    x = x - splats[i][c] * wb[0][c]
                ref[i * PAD : (i + 1) * PAD, :] = x
        else:
            for i in range(side // PAD):
                r = slice(i * PAD, (i + 1) * PAD)
                src = ref[r, pl.ds(column, LANES)]
                splat = [take(src, jnp.full((8, LANES), 0, jnp.int32) + (lane0 + c)) for c in range(reals)]
                for j in range(cols):
                    x = jnp.where(w[j][1], 0.0, ref[r, j * LANES : (j + 1) * LANES])
                    for c in range(reals):
                        x = x - splat[c] * wb[j][c]
                    ref[r, j * LANES : (j + 1) * LANES] = x
        for j in range(cols):
            ref[pl.ds(at, PAD), j * LANES : (j + 1) * LANES] = jnp.where(sub < reals, w[j][0], rows[j])
        return carry

    lax.fori_loop(0, side // PAD, step, 0)


def place(tile, src, dst, width=PAD):
    moved = tile if src == dst else pltpu.roll(tile, (dst - src) % LANES, 1)
    lane = iota((8, LANES), 1)
    return jnp.where((lane >= dst) & (lane < dst + width), moved, 0.0)


def invert(n, sc, recv, dred, qrb, sbb):
    half = n // 2
    side = half * PAD
    cols = side // LANES
    shift = sc[SHIFT]
    layers = n // 16
    qrb[...] = jnp.zeros_like(qrb)
    sbb[...] = jnp.zeros_like(sbb)
    dred[...] = jnp.zeros_like(dred)
    for g in range(n):
        x, y, z = g % 4, g // 4 % 4, g // 16
        k = g // 2
        tile = recv[lax.rem(g + shift, n)]
        at = k * PAD
        own = slice((at // LANES) * LANES, (at // LANES + 1) * LANES)
        diag = place(tile, 0, at % LANES)
        if (x + y + z) % 2 == 0:
            dred[:, own] += diag
            there = (x > 0, x < 3, y > 0, y < 3, z > 0, z < layers - 1)
            parts = {}
            for f, step in enumerate(STEPS):
                if there[f]:
                    to = (g + step) // 2 * PAD
                    piece = place(tile, PAD * (1 + f), to % LANES)
                    parts[to // LANES] = parts[to // LANES] + piece if to // LANES in parts else piece
            for j, v in parts.items():
                qrb[at : at + PAD, j * LANES : (j + 1) * LANES] = v
        else:
            sbb[at : at + PAD, own] = diag
    sub, lane = iota((8, LANES), 0), iota((8, LANES), 1)
    padded = (sub >= 6) & (sub == (lane & 7))
    tred = []
    for j in range(cols):
        m = dred[:, j * LANES : (j + 1) * LANES]
        m = jnp.where(padded, 1.0, m)
        for k in range(6):
            col = take(m, (lane & ~7) + k)
            row = jnp.broadcast_to(m[k : k + 1, :], (8, LANES))
            inv = 1.0 / jnp.broadcast_to(col[k : k + 1, :], (8, LANES))
            scaled = row * inv
            in_col, in_row = (lane & 7) == k, sub == k
            m = jnp.where(
                in_row,
                jnp.where(in_col, inv, scaled),
                jnp.where(in_col, -col * inv, m - col * scaled),
            )
        tred.append(m)
    dd = jnp.concatenate(
        [
            jnp.concatenate([jnp.where((lane + j * LANES) >> 3 == k, tred[j], 0.0) for j in range(cols)], axis=1)
            for k in range(half)
        ],
        axis=0,
    )
    q = qrb[...]
    t = dot(dd, q)
    r, c = iota((side, side), 0), iota((side, side), 1)
    sbb[...] = jnp.where((r == c) & ((r & 7) >= 6), 1.0, sbb[...] - dot(q, t, ((0,), (0,))))
    sweep(sbb, side)
    sinv = -sbb[...]
    ts = dot(t, sinv)
    def slot_of(pos, black):
        twice = 2 * pos
        odd = ((twice >> 2) ^ (twice >> 4)) & 1
        g = twice + ((1 - odd) if black else odd)
        return lax.rem(g + shift, n)

    rr, cc = iota((side, LANES), 0), iota((side, LANES), 1)
    sel = []
    for black in (False, True):
        slot = slot_of(rr >> 3, black)
        hit = jnp.zeros((side, LANES), jnp.bool_)
        for b, step in enumerate((0,) + STEPS):
            hit = hit | ((cc >> 3 == b) & (slot == lax.rem(sc[SLOT] + step + n, n)))
        sel.append(jnp.where(hit & ((rr & 7) == (cc & 7)), 1.0, 0.0).astype(F32))
    upper = dot(dd, sel[0]) + dot(ts, dot(t, sel[0], ((0,), (0,)))) - dot(ts, sel[1])
    lower = dot(sinv, sel[1]) - dot(ts, sel[0], ((0,), (0,)))
    pr, pc = iota((n * PAD, side), 0), iota((n * PAD, side), 1)
    out = None
    for black, x in ((False, upper), (True, lower)):
        onehot = jnp.where((slot_of(pc >> 3, black) == pr >> 3) & ((pc & 7) == (pr & 7)), 1.0, 0.0).astype(F32)
        v = dot(onehot, x)
        out = v if out is None else out + v
    return out


class Product:
    def __init__(self, b_hbm, b_vmem, sems, acc, vec):
        self.b, self.acc, self.vec = b_vmem, acc, vec
        self.chunks, rows = b_vmem.shape[:2]
        self.copy = lambda k: pltpu.make_async_copy(b_hbm.at[0, pl.ds(k * rows, rows), :], b_vmem.at[k], sems.at[k])

    def start(self):
        def one(k, carry):
            self.copy(k).start()
            return carry

        lax.fori_loop(0, self.chunks, one, 0)

    def __call__(self, tiles, code, inv):
        acc, vec = self.acc, self.vec
        blocks = len(tiles)
        moved = permute(lambda b: tiles[b], code, blocks)
        per = blocks // self.chunks
        for k in range(self.chunks):
            v = jnp.concatenate(moved[k * per : (k + 1) * per], axis=1)
            high = v.astype(jnp.bfloat16)
            low = (v - high.astype(F32)).astype(jnp.bfloat16)
            vec[k] = jnp.concatenate([high, low], axis=0)
        for k in range(self.chunks):
            self.copy(k).wait()
            part = dot(vec[k], self.b[k], precision=None)
            acc[...] = part if k == 0 else acc[...] + part
        return permute(lambda b: acc[0:8, b * LANES : (b + 1) * LANES] + acc[8:16, b * LANES : (b + 1) * LANES], inv, blocks)


def lanes_of(ref, b):
    return ref[:, b * LANES : (b + 1) * LANES]


def weigh(fc, f, t, x):
    return jnp.where(fc.shared(f, t), 0.5, jnp.where(fc.live(f, t), 1.0, 0.0)) * x


def total(tiles):
    acc = tiles[0]
    for x in tiles[1:]:
        acc = acc + x
    return jnp.sum(acc, axis=1, keepdims=True)


def coarse_of(n, recv, qloc):
    width = n * PAD
    rows = jnp.concatenate([recv[i] for i in range(n)], axis=0)
    dense = dot(rows, spread(n, width))
    goal = None
    both = None
    for i in range(n):
        x = dense[i * 8 : (i + 1) * 8, :]
        x = x if i == 0 else pltpu.roll(x, i * PAD, 1)
        goal = x if goal is None else goal + x
        both = recv[i] if both is None else both + recv[i]
    return dot(goal, qloc[...])[:, :EXTRA], both


def finish(n, fc, y, extra, c_ref, ybuf, tile_out):
    for b, v in enumerate(y):
        ybuf[:, b * LANES : (b + 1) * LANES] = v
    row = dot(ybuf[...], c_ref[...], ((1,), (1,)))
    tile = jnp.concatenate([row, jnp.zeros((8, LANES - EXTRA), F32)], axis=1)
    lane = iota((8, LANES), 1)
    for k, v in enumerate(extra):
        tile = jnp.where(lane == EXTRA + k, v, tile)
    for i in range(n):
        tile_out[i] = tile


def start_kernel(n, cap, faces, product, sc, recv, c_ref, rhs, code, inv, *refs):
    nm = len(pairings(n)[0])
    lam_out, t_out, q_out, tile_out = refs[:4]
    sends = refs[4 : 4 + nm]
    dred, qrb, sbb = refs[4 + nm :]
    fc = Faces(sc, n, cap)
    blocks = cap * faces // LANES
    q_out[...] = invert(n, sc, recv, dred, qrb, sbb)
    goal = []
    for j in range(n * PAD // LANES):
        v = None
        for i in range(j * (LANES // PAD), (j + 1) * (LANES // PAD)):
            x = place(recv[i], EXTRA, (i * PAD) % LANES)
            v = x if v is None else v + x
        goal.append(v)
    z = dot(jnp.concatenate(goal, axis=1), q_out[...])[:, :EXTRA]
    lam_out[...] = dot(z, c_ref[...])
    y = product([lanes_of(lam_out, b) for b in range(blocks)], code, inv)
    t = [lanes_of(rhs, b) - y[b] for b in range(blocks)]
    fc.send(t, sends)
    finish(n, fc, t, [], c_ref, t_out, tile_out)


def assembled(fc, faces, c_ref, z, y_ref, far, buf):
    buf[...] = dot(z, c_ref[...])
    out = []
    for f in range(faces):
        for t in range(fc.per):
            b = f * fc.per + t
            v = lanes_of(y_ref, b) - fc.far(far, f, t)
            out.append(jnp.where(fc.live(f, t), v, 0.0) - lanes_of(buf, b))
    return out


def step_kernel(n, cap, faces, kind, product, sc, recv, c_ref, q_ref, code, inv, y_ref, *refs):
    refs = list(refs)
    nm = len(pairings(n)[0])
    pop = lambda k: [refs.pop(0) for _ in range(k)]
    far = pop(nm)
    state = pop({0: 0, 1: 2, 2: 5, 3: 5}[kind])
    fc = Faces(sc, n, cap)
    blocks = cap * faces // LANES
    if kind == 3:
        x_out, w_out, buf = refs
    else:
        w_out = pop(1)[0]
        x_out, p_out, s_out, k_out = pop(4) if kind else (None,) * 4
        y_out, tile_out = pop(2)
        sends = pop(nm)
        (buf,) = refs
    z, both = coarse_of(n, recv, q_ref)
    q = assembled(fc, faces, c_ref, z, y_ref, far, buf)
    if kind == 0:
        w, p, s = q, None, None
    else:
        rho, mu = both[:, EXTRA : EXTRA + 1], both[:, EXTRA + 1 : EXTRA + 2]
        w_old = [lanes_of(state[0], b) for b in range(blocks)]
        x_old = [lanes_of(state[1], b) for b in range(blocks)]
        if kind == 1:
            p, s, sigma = w_old, q, mu
        else:
            last = state[4][...]
            beta = rho / last[:, 0:1]
            cross = both[:, EXTRA + 2 : EXTRA + 3]
            sigma = mu + beta * cross + beta * beta * last[:, 1:2]
            p = [w_old[b] + beta * lanes_of(state[2], b) for b in range(blocks)]
            s = [q[b] + beta * lanes_of(state[3], b) for b in range(blocks)]
        alpha = rho / sigma
        w = [w_old[b] - alpha * s[b] for b in range(blocks)]
        x = [x_old[b] + alpha * p[b] for b in range(blocks)]
        if kind == 3:
            for out, v in ((x_out, x), (w_out, w)):
                for b, m in enumerate(permute(lambda b: v[b], code, blocks)):
                    out[0, :, b * LANES : (b + 1) * LANES] = m
            return
        lane = iota((8, LANES), 1)
        k_out[...] = jnp.where(lane == 0, rho, jnp.where(lane == 1, sigma, 0.0))
        for b in range(blocks):
            at = slice(b * LANES, (b + 1) * LANES)
            x_out[:, at], p_out[:, at], s_out[:, at] = x[b], p[b], s[b]
    for b in range(blocks):
        w_out[:, b * LANES : (b + 1) * LANES] = w[b]
    y = product(w, code, inv)
    fc.send(y, sends)
    w = [lanes_of(w_out, b) for b in range(blocks)]
    weighted = [weigh(fc, b // fc.per, b % fc.per, w[b]) for b in range(blocks)]
    extra = [total([weighted[b] * w[b] for b in range(blocks)]), total([w[b] * y[b] for b in range(blocks)])]
    if kind:
        extra.append(total([weighted[b] * lanes_of(s_out, b) + lanes_of(p_out, b) * y[b] for b in range(blocks)]))
    finish(n, fc, y, extra, c_ref, y_out, tile_out)


VMEM = pl.BlockSpec(memory_space=pltpu.VMEM)
SMEM = pl.BlockSpec(memory_space=pltpu.SMEM)
ANY = pl.BlockSpec(memory_space=pl.ANY)


def struct(*shape, dtype=F32):
    return jax.ShapeDtypeStruct(shape, dtype)


def per_device(
    dual_blocks, rigid_modes, dual_local, coarse_rhs, iface_sizes, neighbours, shared_counts, iface_map, owner
):
    n = lax.axis_size("dev")
    faces = neighbours.shape[1]
    nmax = iface_map.shape[1]
    cap = nmax // faces
    modes, loads = coarse_rhs.shape[1:]
    blocks = nmax // LANES
    pairs, _ = pairings(n)
    nm = len(pairs)
    params = pltpu.CompilerParams(vmem_limit_bytes=56 * 1024 * 1024)
    vec = struct(8, nmax)
    face = [struct(8, cap)] * nm
    tiles = struct(n, 8, LANES)
    table = struct(blocks, LANES, dtype=jnp.int32)
    chunk = 256

    def call(body, name, outs, scratch, sc, *args, dense=None):
        stage = [pltpu.SMEM(sc.shape, sc.dtype)] + [pltpu.VMEM(a.shape, a.dtype) for a in args]
        extra = [] if dense is None else [dense]
        streams = [
            pltpu.VMEM((nmax // chunk, chunk, nmax), jnp.bfloat16),
            pltpu.SemaphoreType.DMA((nmax // chunk,)),
            pltpu.VMEM((16, nmax), F32),
            pltpu.VMEM((nmax // chunk, 16, chunk), jnp.bfloat16),
        ]

        def kernel(*refs):
            refs = list(refs)
            pop = lambda k: [refs.pop(0) for _ in range(k)]
            ins, big, results = pop(len(stage)), pop(len(extra)), pop(len(outs))
            local = pop(len(stage))
            (sems,) = pop(1)
            product = Product(big[0], *pop(4)) if big else None
            copies = [pltpu.make_async_copy(a, b, sems.at[i]) for i, (a, b) in enumerate(zip(ins, local))]
            for c in copies:
                c.start()
            if product:
                product.start()
            for c in copies:
                c.wait()
            body(product, *local, *results, *refs)

        return pl.pallas_call(
            kernel,
            out_shape=outs,
            in_specs=[ANY] * (len(stage) + len(extra)),
            out_specs=[VMEM] * len(outs),
            scratch_shapes=stage + [pltpu.SemaphoreType.DMA((len(stage),))] + (streams if extra else []) + scratch,
            compiler_params=params,
            name=name,
        )(sc, *args, *extra)

    def exchange(parts):
        return [lax.ppermute(x, "dev", perm) for x, (_, _, perm) in zip(parts, pairs)]

    def everyone(x):
        return lax.all_to_all(x, "dev", 0, 0)

    outs = [struct(16, dtype=jnp.int32), vec, vec, table, table] + face
    sc, modes_c, rhs_c, code, inv, *send = pl.pallas_call(
        functools.partial(prepare_kernel, n, cap, faces),
        out_shape=outs,
        in_specs=[SMEM] * 4 + [VMEM] * 4,
        out_specs=[SMEM] + [VMEM] * (len(outs) - 1),
        compiler_params=params,
        name="prepare",
    )(
        owner,
        iface_sizes,
        shared_counts,
        neighbours,
        iface_map,
        iface_map.reshape(blocks, LANES),
        rigid_modes.reshape(modes * blocks, LANES),
        dual_local,
    )
    far = exchange(send)
    c_mat, tile = call(
        lambda _, *refs: row_kernel(n, cap, faces, *refs),
        "coarse_row",
        [struct(EXTRA, nmax), tiles],
        [],
        sc,
        modes_c,
        coarse_rhs[0],
        *far,
    )
    recv = everyone(tile)
    side = n * PAD // 2
    x, y, q_mat, tile, *send = call(
        functools.partial(start_kernel, n, cap, faces),
        "start",
        [vec, vec, struct(n * PAD, LANES), tiles] + face,
        [pltpu.VMEM((8, side), F32), pltpu.VMEM((side, side), F32), pltpu.VMEM((side, side), F32)],
        sc,
        recv,
        c_mat,
        rhs_c,
        code,
        inv,
        dense=dual_blocks,
    )
    state = []
    for kind in (0, 1, 2, 3):
        recv, far = everyone(tile), exchange(send)
        args = (sc, recv, c_mat, q_mat, code, inv, y, *far, *state)
        body = functools.partial(step_kernel, n, cap, faces, kind)
        buf = [pltpu.VMEM((8, nmax), F32)]
        if kind == 3:
            return tuple(call(body, "last", [struct(1, 8, nmax)] * 2, buf, *args))
        outs = [vec] + ([vec, vec, vec, struct(8, LANES)] if kind else []) + [vec, tiles] + face
        got = list(call(body, f"step{kind}", outs, buf, *args, dense=dual_blocks))
        w = got.pop(0)
        if kind:
            x, p, s, scal = got[:4]
            got = got[4:]
            state = [w, x, p, s, scal]
        else:
            state = [w, x]
        y, tile, send = got[0], got[1], got[2:]


def solution(mesh):
    return jax.shard_map(
        per_device,
        mesh=mesh,
        in_specs=(
            P("dev", None, None),
            P("dev", None, None),
            P("dev", None, None),
            P("dev", None, None),
            P("dev"),
            P("dev", None),
            P("dev", None),
            P("dev", None),
            P(),
        ),
        out_specs=(P("dev", None, None), P("dev", None, None)),
        check_vma=False,
    )
```

```python
import functools

import jax
import jax.numpy as jnp
from jax import lax
from jax.experimental import pallas as pl
from jax.experimental.pallas import tpu as pltpu
from jax.sharding import PartitionSpec as P

HI = lax.Precision.HIGHEST
F32 = jnp.float32
STEPS = (-1, 1, -4, 4, -16, 16)
LANES = 128
PAD = 8
EXTRA = 64
SLOT, SHIFT, SIZE, COUNT, LINK = 0, 1, 2, 3, 9


def pairings(n):
    out = []
    for axis, dist in enumerate((1, 4, 16)):
        seen = []
        for phase in (0, 1):
            pairs = sorted({tuple(sorted((i, (i + dist) % n))) for i in range(n) if (i // dist) % 2 == phase})
            if pairs in seen:
                continue
            seen.append(pairs)
            out.append((axis, phase, pairs + [(j, i) for i, j in pairs]))
    merged = [sum(1 for a, _, _ in out if a == axis) == 1 for axis in range(3)]
    return out, merged


def dot(a, b, dims=((1,), (0,)), precision=HI):
    return lax.dot_general(a, b, (dims, ((), ())), precision=precision, preferred_element_type=F32)


def iota(shape, dim):
    return lax.broadcasted_iota(jnp.int32, shape, dim)


def take(x, idx):
    return jnp.take_along_axis(x, idx, axis=1, mode="promise_in_bounds")


def permute(load, table, blocks, which=None):
    tiles = [load(b) for b in range(blocks)]
    out = []
    for b in range(blocks) if which is None else which:
        row = jnp.broadcast_to(table[b : b + 1, :], (8, LANES))
        high, low = row >> 7, row & 127
        acc = jnp.zeros((8, LANES), F32)
        for s in range(blocks):
            acc = jnp.where(high == s, take(tiles[s], low), acc)
        out.append(acc)
    return out


class Faces:
    def __init__(self, sc, n, cap):
        self.sc, self.n, self.cap = sc, n, cap
        self.per = cap // LANES
        self.list, self.merged = pairings(n)

    def bit(self, axis):
        return (self.sc[SLOT] >> (0, 2, 4)[axis]) & 1

    def live(self, f, t):
        return iota((8, LANES), 1) + t * LANES < self.sc[COUNT + f]

    def shared(self, f, t):
        return self.live(f, t) & (self.sc[LINK + f] > 0)

    def send(self, tiles, outs):
        for ref, (axis, phase, _) in zip(outs, self.list):
            up = self.sc[LINK + 2 * axis + 1] > 0 if self.merged[axis] else self.bit(axis) == phase
            for t in range(self.per):
                low, high = tiles[2 * axis * self.per + t], tiles[(2 * axis + 1) * self.per + t]
                ref[:, t * LANES : (t + 1) * LANES] = jnp.where(up, high, low)

    def far(self, ins, f, t):
        axis = f // 2
        mine = [ref for ref, (a, _, _) in zip(ins, self.list) if a == axis]
        vals = [ref[:, t * LANES : (t + 1) * LANES] for ref in mine]
        if len(vals) == 1:
            v = vals[0]
        else:
            zero = self.bit(axis) == 0
            v = jnp.where(zero, vals[0], vals[1]) if f % 2 else jnp.where(zero, vals[1], vals[0])
        return jnp.where(self.shared(f, t), v, 0.0)


def spread(n, width):
    row, col = iota((LANES, width), 0), iota((LANES, width), 1)
    hit = jnp.zeros((LANES, width), jnp.bool_)
    for b, step in enumerate((0,) + STEPS):
        hit = hit | ((row >> 3 == b) & (col == (step % n) * PAD + (row & 7)))
    return jnp.where(hit, 1.0, 0.0).astype(jnp.bfloat16)


def halves(x):
    high = x.astype(jnp.bfloat16)
    return high, (x - high.astype(F32)).astype(jnp.bfloat16)


def stacked(x):
    return jnp.concatenate(halves(x), axis=0)


def modes_times(z, c_ref):
    r = dot(stacked(z), c_ref[...], precision=None)
    return r[:8] + r[8:]


def prepare_kernel(n, cap, faces, owner, sizes, counts, links, map_row, map_tile, modes, rhs, sc, *refs):
    nm = len(pairings(n)[0])
    modes_out, rhs_out, code_out, inv_out = refs[:4]
    sends = refs[4 : 4 + nm]
    sc[SLOT] = lax.axis_index("dev").astype(jnp.int32)
    sc[SHIFT] = owner[0]
    sc[SIZE] = sizes[0]
    for f in range(faces):
        sc[COUNT + f] = counts[0, f]
        sc[LINK + f] = (links[0, f] >= 0).astype(jnp.int32)
    nmax = cap * faces
    blocks = nmax // LANES
    size = sc[SIZE]
    j = iota((1, nmax), 1)
    code = jnp.where(j < size, map_row[...], -1)
    place = j + 1
    high, low = code >> 7, code & 127
    rows = -(-blocks // 8) * 8
    group = iota((rows, nmax), 0)
    hit = jnp.broadcast_to(high, (rows, nmax)) == group
    left = jnp.concatenate(
        [
            jnp.where(hit, jnp.broadcast_to(place >> 6, (rows, nmax)), 0).astype(F32),
            jnp.where(hit, jnp.broadcast_to(place & 63, (rows, nmax)), 0).astype(F32),
        ],
        axis=0,
    ).astype(jnp.bfloat16)
    right = jnp.where(jnp.broadcast_to(low, (LANES, nmax)) == iota((LANES, nmax), 0), 1.0, 0.0).astype(jnp.bfloat16)
    both = dot(left, right, ((1,), (1,)), None)
    inv = (both[:rows] * 64.0 + both[rows:]).astype(jnp.int32) - 1
    inv_out[...] = inv[:blocks]
    tile_j = iota((blocks, LANES), 0) * LANES + iota((blocks, LANES), 1)
    code_out[...] = jnp.where(tile_j < size, map_tile[...], -1)
    count = modes.shape[0] // blocks
    rest = jnp.zeros((8 - count, LANES), F32)
    moved = permute(
        lambda b: jnp.concatenate([modes[pl.ds(b, count, blocks), :], rest], axis=0), inv_out, blocks
    )
    for b, v in enumerate(moved):
        modes_out[:, b * LANES : (b + 1) * LANES] = v
    Faces(sc, n, cap).send(moved, sends)
    for b, v in enumerate(permute(lambda b: rhs[0, :, b * LANES : (b + 1) * LANES], inv_out, blocks)):
        rhs_out[:, b * LANES : (b + 1) * LANES] = v


def row_kernel(n, cap, faces, sc, modes, goal, *refs):
    nm = len(pairings(n)[0])
    ins, (c_half, tile_out, c_out) = refs[:nm], refs[nm:]
    fc = Faces(sc, n, cap)
    c_out[...] = jnp.zeros_like(c_out)
    c_out[0:PAD, :] = modes[...]
    for f in range(faces):
        for t in range(fc.per):
            at = f * cap + t * LANES
            c_out[PAD * (1 + f) : PAD * (2 + f), at : at + LANES] = -fc.far(ins, f, t)
    row = dot(modes[...], c_out[...], ((1,), (1,)))
    c_half[...] = stacked(c_out[...])
    count = goal.shape[0]
    onehot = jnp.where(iota((count, LANES), 1) == iota((count, LANES), 0) + EXTRA, 1.0, 0.0).astype(F32)
    tile = jnp.concatenate([row, jnp.zeros((8, LANES - EXTRA), F32)], axis=1) + dot(goal[...], onehot, ((0,), (0,)))
    for i in range(n):
        tile_out[i] = tile


def sweep(ref, side):
    cols = side // LANES
    reals = 6

    def step(b, carry):
        at = pl.multiple_of(b * PAD, PAD)
        column = 0 if cols == 1 else pl.multiple_of((at // LANES) * LANES, LANES)
        lane0 = at - column
        sub, lane = iota((8, LANES), 0), iota((8, LANES), 1)
        rows = [ref[pl.ds(at, PAD), j * LANES : (j + 1) * LANES] for j in range(cols)]
        pivot = rows[0] if cols == 1 else ref[pl.ds(at, PAD), pl.ds(column, LANES)]
        g = [take(pivot, jnp.full((8, LANES), 0, jnp.int32) + (lane0 + c)) for c in range(reals)]
        for k in range(reals):
            top = [jnp.broadcast_to(g[c][k : k + 1, :], (8, LANES)) for c in range(reals)]
            inv = 1.0 / top[k]
            mine = sub == k
            new = []
            for c in range(reals):
                if c == k:
                    new.append(jnp.where(mine, inv, -g[k] * inv))
                else:
                    scaled = top[c] * inv
                    new.append(jnp.where(mine, scaled, g[c] - g[k] * scaled))
            g = new
        w = []
        for j in range(cols):
            acc = jnp.zeros((8, LANES), F32)
            for c in range(reals):
                acc = acc + g[c] * jnp.broadcast_to(rows[j][c : c + 1, :], (8, LANES))
            here = (lane + j * LANES >= at) & (lane + j * LANES < at + reals)
            minus = acc
            for c in range(reals):
                minus = jnp.where(lane + j * LANES == at + c, -g[c], minus)
            w.append((minus, here))
        wb = [[jnp.broadcast_to(w[j][0][c : c + 1, :], (8, LANES)) for c in range(reals)] for j in range(cols)]
        if cols == 1:
            lanes = [jnp.full((8, LANES), 0, jnp.int32) + (lane0 + c) for c in range(reals)]
            olds = [ref[i * PAD : (i + 1) * PAD, :] for i in range(side // PAD)]
            splats = [[take(x, i) for i in lanes] for x in olds]
            for i, x in enumerate(olds):
                x = jnp.where(w[0][1], 0.0, x)
                for c in range(reals):
                    x = x - splats[i][c] * wb[0][c]
                ref[i * PAD : (i + 1) * PAD, :] = x
        else:
            for i in range(side // PAD):
                r = slice(i * PAD, (i + 1) * PAD)
                src = ref[r, pl.ds(column, LANES)]
                splat = [take(src, jnp.full((8, LANES), 0, jnp.int32) + (lane0 + c)) for c in range(reals)]
                for j in range(cols):
                    x = jnp.where(w[j][1], 0.0, ref[r, j * LANES : (j + 1) * LANES])
                    for c in range(reals):
                        x = x - splat[c] * wb[j][c]
                    ref[r, j * LANES : (j + 1) * LANES] = x
        for j in range(cols):
            ref[pl.ds(at, PAD), j * LANES : (j + 1) * LANES] = jnp.where(sub < reals, w[j][0], rows[j])
        return carry

    lax.fori_loop(0, side // PAD, step, 0)


def place(tile, src, dst, width=PAD):
    moved = tile if src == dst else pltpu.roll(tile, (dst - src) % LANES, 1)
    lane = iota((8, LANES), 1)
    return jnp.where((lane >= dst) & (lane < dst + width), moved, 0.0)


def invert(n, sc, recv, dred, qrb, sbb):
    half = n // 2
    side = half * PAD
    cols = side // LANES
    shift = sc[SHIFT]
    layers = n // 16
    qrb[...] = jnp.zeros_like(qrb)
    sbb[...] = jnp.zeros_like(sbb)
    dred[...] = jnp.zeros_like(dred)
    for g in range(n):
        x, y, z = g % 4, g // 4 % 4, g // 16
        k = g // 2
        tile = recv[lax.rem(g + shift, n)]
        at = k * PAD
        own = slice((at // LANES) * LANES, (at // LANES + 1) * LANES)
        diag = place(tile, 0, at % LANES)
        if (x + y + z) % 2 == 0:
            dred[:, own] += diag
            there = (x > 0, x < 3, y > 0, y < 3, z > 0, z < layers - 1)
            parts = {}
            for f, step in enumerate(STEPS):
                if there[f]:
                    to = (g + step) // 2 * PAD
                    piece = place(tile, PAD * (1 + f), to % LANES)
                    parts[to // LANES] = parts[to // LANES] + piece if to // LANES in parts else piece
            for j, v in parts.items():
                qrb[at : at + PAD, j * LANES : (j + 1) * LANES] = v
        else:
            sbb[at : at + PAD, own] = diag
    sub, lane = iota((8, LANES), 0), iota((8, LANES), 1)
    padded = (sub >= 6) & (sub == (lane & 7))
    tred = []
    for j in range(cols):
        m = dred[:, j * LANES : (j + 1) * LANES]
        m = jnp.where(padded, 1.0, m)
        for k in range(6):
            col = take(m, (lane & ~7) + k)
            row = jnp.broadcast_to(m[k : k + 1, :], (8, LANES))
            inv = 1.0 / jnp.broadcast_to(col[k : k + 1, :], (8, LANES))
            scaled = row * inv
            in_col, in_row = (lane & 7) == k, sub == k
            m = jnp.where(
                in_row,
                jnp.where(in_col, inv, scaled),
                jnp.where(in_col, -col * inv, m - col * scaled),
            )
        tred.append(m)
    dd = jnp.concatenate(
        [
            jnp.concatenate([jnp.where((lane + j * LANES) >> 3 == k, tred[j], 0.0) for j in range(cols)], axis=1)
            for k in range(half)
        ],
        axis=0,
    )
    q = qrb[...]
    t = dot(dd, q)
    r, c = iota((side, side), 0), iota((side, side), 1)
    sbb[...] = jnp.where((r == c) & ((r & 7) >= 6), 1.0, sbb[...] - dot(q, t, ((0,), (0,))))
    sweep(sbb, side)
    sinv = -sbb[...]
    ts = dot(t, sinv)
    def slot_of(pos, black):
        twice = 2 * pos
        odd = ((twice >> 2) ^ (twice >> 4)) & 1
        g = twice + ((1 - odd) if black else odd)
        return lax.rem(g + shift, n)

    rr, cc = iota((side, LANES), 0), iota((side, LANES), 1)
    sel = []
    for black in (False, True):
        slot = slot_of(rr >> 3, black)
        hit = jnp.zeros((side, LANES), jnp.bool_)
        for b, step in enumerate((0,) + STEPS):
            hit = hit | (((cc & 63) >> 3 == b) & (slot == lax.rem(sc[SLOT] + step + n, n)))
        sel.append(jnp.where(hit & ((rr & 7) == (cc & 7)), 1.0, 0.0).astype(F32))
    upper = dot(dd, sel[0]) + dot(ts, dot(t, sel[0], ((0,), (0,)))) - dot(ts, sel[1])
    lower = dot(sinv, sel[1]) - dot(ts, sel[0], ((0,), (0,)))
    pr, pc = iota((n * PAD, side), 0), iota((n * PAD, side), 1)
    out = None
    for black, x in ((False, upper), (True, lower)):
        onehot = jnp.where((slot_of(pc >> 3, black) == pr >> 3) & ((pc & 7) == (pr & 7)), 1.0, 0.0).astype(F32)
        v = dot(onehot, x)
        out = v if out is None else out + v
    return out


def across(left, right, size, unit):
    half = max(size // (2 * unit), 0) * unit
    parts = [(0, half), (half, size)] if half else [(0, size)]
    out = None
    for a, b in parts:
        v = dot(left(a, b), right(a, b), ((1,), (1,)), None)
        out = v if out is None else out + v
    return out


class Product:
    def __init__(self, b_hbm, head, b_vmem, sems, acc, vec):
        self.b, self.head, self.acc, self.vec = b_vmem, head, acc, vec
        self.held = head.shape[0] // b_vmem.shape[1]
        self.chunks, self.rows = b_vmem.shape[0] + self.held, b_vmem.shape[1]

        def copy(k):
            rows = pl.ds(k * self.rows, self.rows)
            return pltpu.make_async_copy(b_hbm.at[0, rows, :], b_vmem.at[k - self.held], sems.at[k - self.held])

        self.copy = copy

    def start(self):
        def one(k, carry):
            self.copy(k).start()
            return carry

        lax.fori_loop(self.held, self.chunks, one, 0)

    def __call__(self, tiles, code, inv):
        acc, vec, rows = self.acc, self.vec, self.rows
        blocks = len(tiles)
        per = rows // LANES
        for k in range(self.chunks):
            at, end = k * rows, (k + 1) * rows
            moved = permute(lambda b: tiles[b], code, blocks, range(k * per, (k + 1) * per))
            vec[:, at:end] = stacked(jnp.concatenate(moved, axis=1))
            if k < self.held:
                right = self.head[at:end, :]
            else:
                self.copy(k).wait()
                right = self.b[k - self.held]
            part = dot(vec[:, at:end], right, precision=None)
            acc[...] = acc[...] + part if k else part
        return permute(lambda b: acc[0:8, b * LANES : (b + 1) * LANES] + acc[8:16, b * LANES : (b + 1) * LANES], inv, blocks)


def lanes_of(ref, b):
    return ref[:, b * LANES : (b + 1) * LANES]


def weigh(fc, f, t, x):
    return jnp.where(fc.shared(f, t), 0.5, jnp.where(fc.live(f, t), 1.0, 0.0)) * x


def total(tiles):
    acc = tiles[0]
    for x in tiles[1:]:
        acc = acc + x
    return jnp.sum(acc, axis=1, keepdims=True)


def coarse_of(n, recv, qloc):
    width = n * PAD
    rows = jnp.concatenate([recv[i] for i in range(n)], axis=0)
    high, rest = halves(rows)
    middle, low = halves(rows - high.astype(F32))
    where = spread(n, width)
    dense = dot(jnp.concatenate([high, middle, low], axis=1), jnp.concatenate([where] * 3, axis=0), precision=None)
    goal = None
    both = None
    for i in range(n):
        x = dense[i * 8 : (i + 1) * 8, :]
        x = x if i == 0 else pltpu.roll(x, i * PAD, 1)
        goal = x if goal is None else goal + x
        both = recv[i] if both is None else both + recv[i]
    return dot(goal, qloc[...]), both


def finish(n, y, extra, c_ref, vec, tile_out):
    for b, v in enumerate(y):
        vec[:, b * LANES : (b + 1) * LANES] = stacked(v)
    row = across(lambda a, b: vec[:, a:b], lambda a, b: c_ref[:, a:b], vec.shape[1], 2 * LANES)
    row = row[:8] + row[8:]
    lane = iota((8, LANES), 1)
    tile = jnp.where(lane < EXTRA, row + pltpu.roll(row, EXTRA, 1), 0.0)
    for k, v in enumerate(extra):
        tile = jnp.where(lane == EXTRA + k, v, tile)
    for i in range(n):
        tile_out[i] = tile


def start_kernel(n, cap, faces, product, sc, recv, c_ref, rhs, code, inv, *refs):
    nm = len(pairings(n)[0])
    lam_out, t_out, q_out, tile_out = refs[:4]
    sends = refs[4 : 4 + nm]
    dred, qrb, sbb = refs[4 + nm :]
    fc = Faces(sc, n, cap)
    blocks = cap * faces // LANES
    q_out[...] = invert(n, sc, recv, dred, qrb, sbb)
    goal = []
    for j in range(n * PAD // LANES):
        v = None
        for i in range(j * (LANES // PAD), (j + 1) * (LANES // PAD)):
            x = place(recv[i], EXTRA, (i * PAD) % LANES)
            v = x if v is None else v + x
        goal.append(v)
    z = dot(jnp.concatenate(goal, axis=1), q_out[...])
    lam_out[...] = modes_times(z, c_ref)
    y = product([lanes_of(lam_out, b) for b in range(blocks)], code, inv)
    t = [lanes_of(rhs, b) - y[b] for b in range(blocks)]
    fc.send(t, sends)
    for b in range(blocks):
        t_out[:, b * LANES : (b + 1) * LANES] = t[b]
    finish(n, t, [], c_ref, product.vec, tile_out)


def assembled(fc, faces, c_ref, z, y_ref, far, buf):
    buf[...] = modes_times(z, c_ref)
    out = []
    for f in range(faces):
        for t in range(fc.per):
            b = f * fc.per + t
            v = lanes_of(y_ref, b) - fc.far(far, f, t)
            out.append(jnp.where(fc.live(f, t), v, 0.0) - lanes_of(buf, b))
    return out


def step_kernel(n, cap, faces, kind, product, sc, recv, c_ref, q_ref, code, inv, y_ref, *refs):
    refs = list(refs)
    nm = len(pairings(n)[0])
    pop = lambda k: [refs.pop(0) for _ in range(k)]
    far = pop(nm)
    state = pop({0: 0, 1: 2, 2: 5, 3: 5}[kind])
    fc = Faces(sc, n, cap)
    blocks = cap * faces // LANES
    if kind == 3:
        x_out, w_out, buf = refs
    else:
        w_out = pop(1)[0]
        x_out, p_out, s_out, k_out = pop(4) if kind else (None,) * 4
        y_out, tile_out = pop(2)
        sends = pop(nm)
        (buf,) = refs
    z, both = coarse_of(n, recv, q_ref)
    q = assembled(fc, faces, c_ref, z, y_ref, far, buf)
    if kind == 0:
        w, p, s = q, None, None
    else:
        rho, mu = both[:, EXTRA : EXTRA + 1], both[:, EXTRA + 1 : EXTRA + 2]
        w_old = [lanes_of(state[0], b) for b in range(blocks)]
        x_old = [lanes_of(state[1], b) for b in range(blocks)]
        if kind == 1:
            p, s, sigma = w_old, q, mu
        else:
            last = state[4][...]
            beta = rho / last[:, 0:1]
            cross = both[:, EXTRA + 2 : EXTRA + 3]
            sigma = mu + beta * cross + beta * beta * last[:, 1:2]
            p = [w_old[b] + beta * lanes_of(state[2], b) for b in range(blocks)]
            s = [q[b] + beta * lanes_of(state[3], b) for b in range(blocks)]
        alpha = rho / sigma
        w = [w_old[b] - alpha * s[b] for b in range(blocks)]
        x = [x_old[b] + alpha * p[b] for b in range(blocks)]
        if kind == 3:
            for out, v in ((x_out, x), (w_out, w)):
                for b, m in enumerate(permute(lambda b: v[b], code, blocks)):
                    out[0, :, b * LANES : (b + 1) * LANES] = m
            return
        lane = iota((8, LANES), 1)
        k_out[...] = jnp.where(lane == 0, rho, jnp.where(lane == 1, sigma, 0.0))
        for b in range(blocks):
            at = slice(b * LANES, (b + 1) * LANES)
            x_out[:, at], p_out[:, at], s_out[:, at] = x[b], p[b], s[b]
    for b in range(blocks):
        w_out[:, b * LANES : (b + 1) * LANES] = w[b]
    y = product(w, code, inv)
    fc.send(y, sends)
    w = [lanes_of(w_out, b) for b in range(blocks)]
    weighted = [weigh(fc, b // fc.per, b % fc.per, w[b]) for b in range(blocks)]
    extra = [total([weighted[b] * w[b] for b in range(blocks)]), total([w[b] * y[b] for b in range(blocks)])]
    if kind:
        extra.append(total([weighted[b] * lanes_of(s_out, b) + lanes_of(p_out, b) * y[b] for b in range(blocks)]))
    for b in range(blocks):
        y_out[:, b * LANES : (b + 1) * LANES] = y[b]
    finish(n, y, extra, c_ref, product.vec, tile_out)


VMEM = pl.BlockSpec(memory_space=pltpu.VMEM)
SMEM = pl.BlockSpec(memory_space=pltpu.SMEM)
ANY = pl.BlockSpec(memory_space=pl.ANY)


def struct(*shape, dtype=F32):
    return jax.ShapeDtypeStruct(shape, dtype)


def per_device(
    dual_blocks, rigid_modes, dual_local, coarse_rhs, iface_sizes, neighbours, shared_counts, iface_map, owner
):
    n = lax.axis_size("dev")
    faces = neighbours.shape[1]
    nmax = iface_map.shape[1]
    cap = nmax // faces
    modes, loads = coarse_rhs.shape[1:]
    blocks = nmax // LANES
    pairs, _ = pairings(n)
    nm = len(pairs)
    params = pltpu.CompilerParams(vmem_limit_bytes=56 * 1024 * 1024)
    vec = struct(8, nmax)
    face = [pltpu.VMEM((8, cap), F32)] * nm
    tiles = struct(n, 8, LANES)
    table = struct(blocks, LANES, dtype=jnp.int32)
    chunk = 256
    held = 2
    head = pltpu.with_memory_space_constraint(dual_blocks[0, : held * chunk], pltpu.VMEM)

    def call(body, name, outs, scratch, sc, *args, dense=None, near=()):
        far_args = [a for i, a in enumerate(args) if i not in near]
        near_args = [pltpu.with_memory_space_constraint(args[i], pltpu.VMEM) for i in near]
        stage = [pltpu.SMEM(sc.shape, sc.dtype)] + [pltpu.VMEM(a.shape, a.dtype) for a in far_args]
        extra = [] if dense is None else [dense, head]
        streams = [
            pltpu.VMEM((nmax // chunk - held, chunk, nmax), jnp.bfloat16),
            pltpu.SemaphoreType.DMA((nmax // chunk - held,)),
            pltpu.VMEM((16, nmax), F32),
            pltpu.VMEM((16, nmax), jnp.bfloat16),
        ]

        def kernel(*refs):
            refs = list(refs)
            pop = lambda k: [refs.pop(0) for _ in range(k)]
            ins, big, close, results = pop(len(stage)), pop(len(extra)), pop(len(near)), pop(len(outs))
            local = pop(len(stage))
            (sems,) = pop(1)
            product = Product(*big, *pop(4)) if big else None
            copies = [pltpu.make_async_copy(a, b, sems.at[i]) for i, (a, b) in enumerate(zip(ins, local))]
            for c in copies:
                c.start()
            if product:
                product.start()
            for c in copies:
                c.wait()
            for i, ref in zip(near, close):
                local.insert(i + 1, ref)
            body(product, *local, *results, *refs)

        return pl.pallas_call(
            kernel,
            out_shape=outs,
            in_specs=[ANY] * len(stage) + [ANY, VMEM][: len(extra)] + [VMEM] * len(near),
            out_specs=[VMEM] * len(outs),
            scratch_shapes=stage + [pltpu.SemaphoreType.DMA((len(stage),))] + (streams if extra else []) + scratch,
            compiler_params=params,
            name=name,
        )(sc, *far_args, *extra, *near_args)

    def exchange(parts):
        return [lax.ppermute(x, "dev", perm) for x, (_, _, perm) in zip(parts, pairs)]

    def everyone(x):
        return lax.all_to_all(x, "dev", 0, 0)

    outs = [struct(16, dtype=jnp.int32), vec, vec, table, table] + face
    sc, modes_c, rhs_c, code, inv, *send = pl.pallas_call(
        functools.partial(prepare_kernel, n, cap, faces),
        out_shape=outs,
        in_specs=[SMEM] * 4 + [VMEM] * 4,
        out_specs=[SMEM] + [VMEM] * (len(outs) - 1),
        compiler_params=params,
        name="prepare",
    )(
        owner,
        iface_sizes,
        shared_counts,
        neighbours,
        iface_map,
        iface_map.reshape(blocks, LANES),
        rigid_modes.reshape(modes * blocks, LANES),
        dual_local,
    )
    far = exchange(send)
    c_mat, tile = call(
        lambda _, *refs: row_kernel(n, cap, faces, *refs),
        "coarse_row",
        [struct(2 * EXTRA, nmax, dtype=jnp.bfloat16), tiles],
        [pltpu.VMEM((EXTRA, nmax), F32)],
        sc,
        modes_c,
        coarse_rhs[0],
        *far,
        near=tuple(range(2, 2 + nm)),
    )
    recv = everyone(tile)
    side = n * PAD // 2
    x, y, q_mat, tile, *send = call(
        functools.partial(start_kernel, n, cap, faces),
        "start",
        [vec, vec, struct(n * PAD, LANES), tiles] + face,
        [pltpu.VMEM((8, side), F32), pltpu.VMEM((side, side), F32), pltpu.VMEM((side, side), F32)],
        sc,
        recv,
        c_mat,
        rhs_c,
        code,
        inv,
        dense=dual_blocks,
        near=(0,),
    )
    state = []
    for kind in (0, 1, 2, 3):
        recv, far = everyone(tile), exchange(send)
        args = (sc, recv, c_mat, q_mat, code, inv, y, *far, *state)
        body = functools.partial(step_kernel, n, cap, faces, kind)
        buf = [pltpu.VMEM((8, nmax), F32)]
        near = (0,) + tuple(range(6, 6 + nm))
        if kind == 3:
            return tuple(call(body, "last", [struct(1, 8, nmax)] * 2, buf, *args, near=near))
        outs = [vec] + ([vec, vec, vec, struct(8, LANES)] if kind else []) + [vec, tiles] + face
        got = list(call(body, f"step{kind}", outs, buf, *args, dense=dual_blocks, near=near))
        w = got.pop(0)
        if kind:
            x, p, s, scal = got[:4]
            got = got[4:]
            state = [w, x, p, s, scal]
        else:
            state = [w, x]
        y, tile, send = got[0], got[1], got[2:]


def solution(mesh):
    return jax.shard_map(
        per_device,
        mesh=mesh,
        in_specs=(
            P("dev", None, None),
            P("dev", None, None),
            P("dev", None, None),
            P("dev", None, None),
            P("dev"),
            P("dev", None),
            P("dev", None),
            P("dev", None),
            P(),
        ),
        out_specs=(P("dev", None, None), P("dev", None, None)),
        check_vma=False,
    )
```
